32 devices in a mesh: dp: 16 (over z, y, x), tensor: 2 (over core).
Axes of the slice: x: 2, y: 2, z: 4, core: 2. Of those that a mesh axis runs over, the one named last changes fastest.
Arguments:
- queries: bfloat16 [2048, 4096], P('dp', 'tensor'), may hold values from -4 to 4
- cached_key_rows: bfloat16 [32, 1024, 1024], P('dp', None, 'tensor'), may hold values from -1 to 1
- cached_value_rows: bfloat16 [32, 1024, 1024], P('dp', None, 'tensor'), may hold values from -6 to 6
- parent_ids: int32 [2048], P('dp'), may hold values from 0 to 31, as said below
- lengths: int32 [32], P('dp'), may hold values from 128 to 1024
- residual: bfloat16 [2048, 2048], P('dp', 'tensor'), may hold values from -4 to 4
- out_weight: bfloat16 [4096, 2048], P('tensor'), may hold values from -0.09375 to 0.09375
Outputs:
- mixed_out: bfloat16 [2048, 2048], P('dp', 'tensor')
The draws below stay inside these ranges and needn't reach their ends.
Inputs may be any that keep to these rules, and one draw needn't show every extreme that they name: `parent_ids`: among the 128 children of one index of dp (aligned blocks), at most 16 have parents of one owner; in every draw one owner has exactly 16 children from every block.
All inputs are finite; a program needn't handle non-finite values.
Results may differ from the reference program's by a relative error of at most 0.0044.
Values may be sent and summed in bfloat16 or wider, within the bound.
A program may use at most 64 MiB of HBM per device.

```python
import math
import jax
import jax.numpy as jnp
from jax import lax

QUERY_HEADS = 32
KEY_VALUE_HEADS = 8
HEAD_WIDTH = 128
W = 2048
CH_DEV = 128
LONGEST_PREFIX = 1024
PAR_DEV = 2
CAP = 16
CHILDREN = 2048
PARENT_COUNT = 32


def draw_parent_ids(key, part):
    owner_count = PARENT_COUNT // PAR_DEV
    first_key, second_key = jax.random.split(jax.random.fold_in(key, 11))
    busy_owner = jax.random.randint(first_key, (), 0, owner_count)

    def one_block(block_key):
        perm_key, order_key, sub_key = jax.random.split(block_key, 3)
        tokens = jax.random.permutation(perm_key, (owner_count - 1) * CAP)[:CH_DEV - CAP]
        others = tokens // CAP
        others = others + (others >= busy_owner).astype(jnp.int32)
        owners = jnp.concatenate([jnp.full((CAP,), busy_owner, jnp.int32), others.astype(jnp.int32)])
        owners = jax.random.permutation(order_key, owners)
        sub_index = jax.random.randint(sub_key, (CH_DEV,), 0, PAR_DEV)
        return owners * PAR_DEV + sub_index
    block_keys = jax.random.split(second_key, owner_count)
    return jax.vmap(one_block)(block_keys).reshape(-1).astype(jnp.int32)


def draw_lengths(key, part):
    first_key, second_key = jax.random.split(jax.random.fold_in(key, 29))
    prefix_lengths = jax.random.randint(first_key, (PARENT_COUNT,), LONGEST_PREFIX // 8, LONGEST_PREFIX + 1)
    longest = jax.random.randint(second_key, (), 0, PARENT_COUNT)
    prefix_lengths = jnp.where(jnp.arange(PARENT_COUNT) == longest, LONGEST_PREFIX, prefix_lengths)
    return prefix_lengths.astype(jnp.int32)


def levels(own_key, shape, cuts, smallest, high):
    def one(axis_at, parts):
        draws = jax.random.uniform(jax.random.fold_in(jax.random.fold_in(own_key, 6), axis_at), (parts,), jnp.float32, smallest / len(cuts), high / len(cuts))
        return jnp.repeat(jnp.exp(draws), shape[axis_at] // parts).reshape((-1,) + (1,) * (len(shape) - axis_at - 1))

    factor_of = one(*cuts[0])
    for cut in cuts[1:]:
        factor_of = factor_of * one(*cut)
    return factor_of


def gaussian(stream_key, shape, scale, most, shards=(), held_as=jnp.bfloat16):
    level = levels(stream_key, shape, shards, -0.22, 0.18) if shards else 1.0
    result = jax.random.normal(stream_key, shape, jnp.float32) * scale * level
    return jnp.minimum(jnp.maximum(result, -most), most).astype(held_as)


def setup_inputs(seed: int = 0) -> dict:
    seeds = jax.random.split(jax.random.key(seed), 8)
    queries = jnp.clip(jax.random.uniform(seeds[0], (CHILDREN, QUERY_HEADS * HEAD_WIDTH), jnp.float32, -4.0, 4.0) * levels(seeds[0], (CHILDREN, QUERY_HEADS * HEAD_WIDTH), ((0, 16), (1, 2)), -0.4, 0.0), -4.0, 4.0).astype(jnp.bfloat16)
    cached_key_rows = jnp.clip(jax.random.uniform(seeds[1], (PARENT_COUNT, LONGEST_PREFIX, KEY_VALUE_HEADS * HEAD_WIDTH), jnp.float32, -1.0, 1.0) * levels(seeds[1], (PARENT_COUNT, LONGEST_PREFIX, KEY_VALUE_HEADS * HEAD_WIDTH), ((0, 16), (2, 2)), -0.4, 0.0), -1.0, 1.0).astype(jnp.bfloat16)
    cached_value_rows = gaussian(seeds[2], (PARENT_COUNT, LONGEST_PREFIX, KEY_VALUE_HEADS * HEAD_WIDTH), 1.0, 6.0, ((0, 16), (2, 2)))
    parent_ids = draw_parent_ids(jax.random.fold_in(seeds[7], 71), 0)
    lengths = draw_lengths(jax.random.fold_in(seeds[7], 71), 0)
    residual = gaussian(seeds[5], (CHILDREN, W), 0.5, 4.0, ((0, 16), (1, 2)))
    out_weight = gaussian(seeds[6], (QUERY_HEADS * HEAD_WIDTH, W), (QUERY_HEADS * HEAD_WIDTH) ** -0.5, 0.09375, ((0, 2),))
    return dict(queries=queries, cached_key_rows=cached_key_rows, cached_value_rows=cached_value_rows, parent_ids=parent_ids, lengths=lengths, residual=residual, out_weight=out_weight)


def reference(queries, cached_key_rows, cached_value_rows, parent_ids, lengths, residual, out_weight):
    group_width = QUERY_HEADS // KEY_VALUE_HEADS
    score_scale = 1.0 / math.sqrt(HEAD_WIDTH)
    block_length = math.gcd(CHILDREN, 64)
    positions = jnp.arange(LONGEST_PREFIX, dtype=jnp.int32)

    def attend(operands):
        query_matrix, parent_nodes = operands
        key_matrix = cached_key_rows[parent_nodes].astype(jnp.float32).reshape(block_length, LONGEST_PREFIX, KEY_VALUE_HEADS, HEAD_WIDTH)
        value_matrix = cached_value_rows[parent_nodes].astype(jnp.float32).reshape(block_length, LONGEST_PREFIX, KEY_VALUE_HEADS, HEAD_WIDTH)
        limits = lengths[parent_nodes]
        query_head_count = query_matrix.astype(jnp.float32).reshape(block_length, KEY_VALUE_HEADS, group_width, HEAD_WIDTH)
        scores = jnp.einsum('bjgd,bljd->bjgl', query_head_count, key_matrix) * score_scale
        live_mask = positions[None, :] < limits[:, None]
        raised = jnp.where(live_mask[:, None, None, :], jnp.exp(scores), jnp.zeros((), jnp.float32))
        totals = lax.optimization_barrier(jnp.sum(raised, axis=-1))
        rounded = lax.optimization_barrier(raised.astype(jnp.bfloat16)).astype(jnp.float32)
        summed = jnp.einsum('bjgl,bljd->bjgd', rounded, value_matrix)
        return (summed / totals[..., None]).reshape(block_length, QUERY_HEADS * HEAD_WIDTH).astype(jnp.bfloat16)
    attended = lax.map(attend, (queries.reshape(CHILDREN // block_length, block_length, QUERY_HEADS * HEAD_WIDTH), parent_ids.reshape(CHILDREN // block_length, block_length)))
    attended = attended.reshape(CHILDREN, QUERY_HEADS * HEAD_WIDTH)
    mixed_out = residual.astype(jnp.float32) + jnp.dot(attended, out_weight, preferred_element_type=jnp.float32)
    return mixed_out.astype(jnp.bfloat16)
```

```python
import functools
import math

import jax
import jax.numpy as jnp
from jax import lax
from jax.experimental import pallas as pl
from jax.experimental.pallas import tpu as pltpu
from jax.sharding import PartitionSpec as P

HEAD_WIDTH = 128


def attend(rows, key_block, value_block, prefix_length, kv_heads):
    slot_total, columns = rows.shape
    group_width = columns // (kv_heads * HEAD_WIDTH)
    prefix_span = key_block.shape[0]
    query_head_count = rows.reshape(slot_total, kv_heads, group_width, HEAD_WIDTH)
    key_heads = key_block.reshape(prefix_span, kv_heads, HEAD_WIDTH)
    value_heads = value_block.reshape(prefix_span, kv_heads, HEAD_WIDTH)
    scores = jnp.einsum(
        "sjgd,ljd->jsgl", query_head_count, key_heads, preferred_element_type=jnp.float32
    )
    scores = scores * (1.0 / math.sqrt(HEAD_WIDTH))
    live_mask = jnp.arange(prefix_span, dtype=jnp.int32) < prefix_length
    raised = jnp.where(live_mask, jnp.exp(scores), jnp.zeros((), jnp.float32))
    totals = jnp.sum(raised, axis=-1)
    summed = jnp.einsum(
        "jsgl,ljd->sjgd",
        raised.astype(jnp.bfloat16),
        value_heads,
        preferred_element_type=jnp.float32,
    )
    scaled = summed / jnp.transpose(totals, (1, 0, 2))[..., None]
    return scaled.reshape(slot_total, columns).astype(jnp.bfloat16)

PLANE = 4
MESH = pl.DeviceIdType.MESH
VMEM_MB = 58


def SEND_ORDER(planes):
    return [g ^ (g >> 1) for g in range(planes)]


def flip(number, mask, bits):
    total = 0
    for bit in range(bits):
        unit = 1 << bit
        total = total + ((number // unit) % 2 + (mask // unit) % 2) % 2 * unit
    return total


def exchange_kernel(
    n, query_hbm, key_hbm, value_hbm, id_hbm, length_hbm, residual_hbm, weight_hbm, mixed_ref,
    queries, keys, values, weight, residual, lengths, ids, outgoing, landed, result, back,
    part_out, part_in, take, fetch_sem, id_send, id_recv, send_sem, recv_sem,
    part_send, part_recv, back_send, back_recv,
):
    me = lax.axis_index("dp")
    core = lax.axis_index("tensor")
    partner = 1 - core
    planes = n // PLANE
    bits = planes.bit_length() - 1
    my_plane, my_seat = me // PLANE, me % PLANE
    children, columns = queries.shape
    capacity = outgoing.shape[1]
    parents, span, _ = keys.shape
    kv_heads = keys.shape[2] // HEAD_WIDTH
    half = residual.shape[1]
    group = columns // (kv_heads * HEAD_WIDTH)
    rows = PLANE * capacity
    slots = n * capacity

    fetches = [
        pltpu.make_async_copy(source, target, fetch_sem.at[i])
        for i, (source, target) in enumerate(
            [
                (id_hbm, ids.at[me]),
                (query_hbm, queries),
                (length_hbm, lengths),
                (key_hbm, keys),
                (value_hbm, values),
                (weight_hbm, weight),
                (residual_hbm, residual),
            ]
        )
    ]
    for fetch in fetches[:2]:
        fetch.start()

    barrier = pltpu.get_barrier_semaphore()
    for step in range(1, n):
        pl.semaphore_signal(
            barrier, inc=1, device_id=((me + step) % n, core), device_id_type=MESH
        )
    pl.semaphore_signal(barrier, inc=1, device_id=(me, partner), device_id_type=MESH)
    for fetch in fetches[2:]:
        fetch.start()

    def id_copy(target, slot):
        return pltpu.make_async_remote_copy(
            src_ref=ids.at[me],
            dst_ref=ids.at[slot],
            send_sem=id_send.at[target],
            recv_sem=id_recv.at[slot],
            device_id=(target, core),
            device_id_type=MESH,
        )

    def query_copy(target, slot):
        return pltpu.make_async_remote_copy(
            src_ref=outgoing.at[target],
            dst_ref=landed.at[slot],
            send_sem=send_sem.at[target],
            recv_sem=recv_sem.at[slot],
            device_id=(target, core),
            device_id_type=MESH,
        )

    def back_copy(target, slot):
        return pltpu.make_async_remote_copy(
            src_ref=result.at[target],
            dst_ref=back.at[slot],
            send_sem=back_send.at[target],
            recv_sem=back_recv.at[slot],
            device_id=(target, core),
            device_id_type=MESH,
        )

    def part_copy(g):
        return pltpu.make_async_remote_copy(
            src_ref=part_out.at[g],
            dst_ref=part_in.at[g],
            send_sem=part_send.at[g],
            recv_sem=part_recv.at[g],
            device_id=(me, partner),
            device_id_type=MESH,
        )

    fetches[0].wait()
    square = (children, children)
    across = jnp.broadcast_to(ids[me].astype(jnp.float32), square)
    down = across.T
    owner_across = jnp.floor((across + 0.5) * (1.0 / parents))
    owner_down = jnp.floor((down + 0.5) * (1.0 / parents))
    row_at = lax.broadcasted_iota(jnp.int32, square, 0)
    column_at = lax.broadcasted_iota(jnp.int32, square, 1)
    zero, one = jnp.zeros(square, jnp.float32), jnp.ones(square, jnp.float32)
    kin = owner_across == owner_down
    alike = jnp.where(across == down, one, zero)
    lower = jnp.where(column_at < row_at, alike, zero)
    upper = jnp.where(row_at < column_at, alike, zero)
    before_down = jnp.where(kin, jnp.where(across < down, one, lower), zero)
    before_across = jnp.where(kin, jnp.where(down < across, one, upper), zero)
    slot_down = owner_down[:, :1] * capacity + jnp.sum(before_down, axis=1, keepdims=True)
    slot_across = owner_across[:1] * capacity + jnp.sum(before_across, axis=0, keepdims=True)
    place = jnp.where(
        lax.broadcasted_iota(jnp.int32, (slots, children), 0).astype(jnp.float32) == slot_across,
        jnp.ones((slots, children), jnp.float32),
        jnp.zeros((slots, children), jnp.float32),
    ).astype(jnp.bfloat16)
    take[...] = jnp.where(
        lax.broadcasted_iota(jnp.int32, (children, slots), 1).astype(jnp.float32) == slot_down,
        jnp.ones((children, slots), jnp.float32),
        jnp.zeros((children, slots), jnp.float32),
    ).astype(jnp.bfloat16)
    fetches[1].wait()
    outgoing[...] = (
        jnp.dot(place, queries[...], preferred_element_type=jnp.float32)
        .astype(jnp.bfloat16)
        .reshape(n, capacity, columns)
    )
    pl.semaphore_wait(barrier, n)

    for step in range(1, n):
        id_copy((me + step) % n, me).start()
    for mask in SEND_ORDER(planes):
        for i in range(PLANE):
            if mask or i:
                target = flip(my_plane, mask, bits) * PLANE + flip(my_seat, i, 2)
                query_copy(target, me).start()
    landed[me] = outgoing[me]
    for fetch in fetches[2:]:
        fetch.wait()
    for step in range(1, n):
        other = (me + step) % n
        id_copy(other, other).wait_recv()
    scale = math.log2(math.e) / math.sqrt(HEAD_WIDTH)

    @pl.loop(0, planes)
    def _(g):
        mask = flip(g, g // 2, bits)
        plane = flip(my_plane, mask, bits)
        seats = [plane * PLANE + flip(my_seat, i, 2) for i in range(PLANE)]

        @pl.when(g > 0)
        def _():
            query_copy(seats[0], seats[0]).wait_recv()

        for i in range(1, PLANE):
            query_copy(seats[i], seats[i]).wait_recv()

        base = plane * PLANE
        spot = lax.broadcasted_iota(jnp.int32, (capacity, 1), 0).astype(jnp.float32)
        tag_parts = []
        for i in range(PLANE):
            known = ids[base + i]
            number = jnp.zeros((capacity, 1), jnp.float32)
            for p in range(parents - 1):
                smaller = jnp.where(
                    known >= me * parents, jnp.where(known <= me * parents + p, 1.0, 0.0), 0.0
                )
                count = jnp.sum(smaller, axis=1, keepdims=True)
                number = number + jnp.where(spot >= count, 1.0, 0.0)
            tag_parts.append(number)
        tags = jnp.concatenate(tag_parts * group, axis=0)
        belongs = [tags == float(p) for p in range(parents)]
        limit = jnp.full(tags.shape, lengths[parents - 1], jnp.int32)
        for p in range(parents - 1):
            limit = jnp.where(belongs[p], lengths[p], limit)
        live = lax.broadcasted_iota(jnp.int32, (rows * group, span), 1) < limit
        pieces = []
        for j in range(kv_heads):
            at = j * HEAD_WIDTH
            q = jnp.concatenate(
                [
                    landed[
                        pl.ds(base, PLANE), :, (j * group + h) * HEAD_WIDTH:(j * group + h + 1) * HEAD_WIDTH
                    ].reshape(rows, HEAD_WIDTH)
                    for h in range(group)
                ],
                axis=0,
            )
            spread = jnp.concatenate(
                [jnp.where(belongs[p], q, jnp.zeros_like(q)) for p in range(parents)], axis=1
            )
            key_pair = jnp.concatenate(
                [keys[p, :, at:at + HEAD_WIDTH] for p in range(parents)], axis=1
            )
            scores = lax.dot_general(
                spread, key_pair, (((1,), (1,)), ((), ())), preferred_element_type=jnp.float32
            )
            raised = jnp.where(live, jnp.exp2(scores * scale), 0.0)
            totals = jnp.sum(raised, axis=1, keepdims=True)
            soft = raised.astype(jnp.bfloat16)
            value_pair = jnp.concatenate(
                [values[p, :, at:at + HEAD_WIDTH] for p in range(parents)], axis=1
            )
            both = jnp.dot(soft, value_pair, preferred_element_type=jnp.float32)
            summed = both[:, (parents - 1) * HEAD_WIDTH:]
            for p in range(parents - 1):
                summed = jnp.where(
                    belongs[p], both[:, p * HEAD_WIDTH:(p + 1) * HEAD_WIDTH], summed
                )
            answer = (summed / totals).astype(jnp.bfloat16)
            pieces += [answer[h * rows:(h + 1) * rows] for h in range(group)]
        attended = jnp.concatenate(pieces, axis=1)
        theirs = pl.multiple_of(partner * half, HEAD_WIDTH)
        mine = pl.multiple_of(core * half, HEAD_WIDTH)
        part_out[g] = jnp.dot(
            attended, weight[:, pl.ds(theirs, half)], preferred_element_type=jnp.float32
        ).astype(jnp.bfloat16)
        part_copy(g).start()
        own = jnp.dot(
            attended, weight[:, pl.ds(mine, half)], preferred_element_type=jnp.float32
        )
        part_copy(g).wait_recv()
        total = (own + part_in[g].astype(jnp.float32)).astype(jnp.bfloat16)
        result[pl.ds(base, PLANE)] = total.reshape(PLANE, capacity, half)

        @pl.when(g > 0)
        def _():
            back_copy(seats[0], me).start()

        for i in range(1, PLANE):
            back_copy(seats[i], me).start()

    back[me] = result[me]
    for step in range(1, n):
        other = (me + step) % n
        id_copy(other, me).wait_send()
        query_copy(other, me).wait_send()
        back_copy(other, me).wait_send()
        back_copy(other, other).wait_recv()
    for g in range(planes):
        part_copy(g).wait_send()
    mixed = jnp.dot(
        take[...], back[...].reshape(slots, half), preferred_element_type=jnp.float32
    )
    mixed_ref[...] = (residual[...].astype(jnp.float32) + mixed).astype(jnp.bfloat16)


def exchange(n, capacity, queries, cached_key_rows, cached_value_rows, parent_ids, lengths, residual, out_weight):
    children, columns = queries.shape
    half = residual.shape[1]
    planes = n // PLANE
    anywhere = pl.BlockSpec(memory_space=pltpu.HBM)
    rows = PLANE * capacity
    dma = pltpu.SemaphoreType.DMA

    def held(*shape):
        return pltpu.VMEM(shape, jnp.bfloat16)

    return pl.pallas_call(
        functools.partial(exchange_kernel, n),
        out_shape=jax.ShapeDtypeStruct(residual.shape, jnp.bfloat16),
        in_specs=[anywhere] * 7,
        out_specs=pl.BlockSpec(memory_space=pltpu.VMEM),
        scratch_shapes=[
            held(*queries.shape),
            held(*cached_key_rows.shape),
            held(*cached_value_rows.shape),
            held(*out_weight.shape),
            held(*residual.shape),
            pltpu.SMEM(lengths.shape, jnp.int32),
            pltpu.VMEM((n, 1, children), jnp.int32),
            held(n, capacity, columns),
            held(n, capacity, columns),
            held(n, capacity, half),
            held(n, capacity, half),
            held(planes, rows, half),
            held(planes, rows, half),
            held(children, n * capacity),
            dma((7,)), dma((n,)), dma((n,)), dma((n,)), dma((n,)),
            dma((planes,)), dma((planes,)), dma((n,)), dma((n,)),
        ],
        compiler_params=pltpu.CompilerParams(
            collective_id=0, has_side_effects=True, vmem_limit_bytes=VMEM_MB << 20
        ),
    )(queries, cached_key_rows, cached_value_rows, parent_ids.reshape(1, children), lengths, residual, out_weight)


def local(queries, cached_key_rows, cached_value_rows, parent_ids, lengths, residual, out_weight):
    dp_count = lax.axis_size("dp")
    children = queries.shape[0]
    columns = queries.shape[1]
    kv_heads = cached_key_rows.shape[2] // HEAD_WIDTH
    parents_here = lengths.shape[0]
    capacity = max(2, 2 * children // dp_count)
    half = residual.shape[1]
    tensor_count = lax.axis_size("tensor")
    planes = dp_count // PLANE
    if (
        capacity % 16 == 0
        and children % 128 == 0
        and dp_count % PLANE == 0
        and planes & (planes - 1) == 0
        and tensor_count == 2
    ):
        return exchange(
            dp_count, capacity, queries, cached_key_rows, cached_value_rows, parent_ids, lengths, residual, out_weight
        )
    owner_of = parent_ids // parents_here
    sub_index = parent_ids % parents_here
    slot_count = dp_count * capacity
    order_rows = jnp.arange(children, dtype=jnp.int32)
    earlier = (owner_of[:, None] == owner_of[None, :]) & (order_rows[:, None] > order_rows[None, :])
    slot_rank = jnp.sum(earlier.astype(jnp.int32), axis=1)
    slot_of = owner_of * capacity + slot_rank
    placing = jnp.arange(slot_count, dtype=jnp.int32)[:, None] == slot_of[None, :]
    placing_rows = placing.astype(jnp.bfloat16)
    tag = jnp.broadcast_to((sub_index + 1)[:, None], (children, HEAD_WIDTH)).astype(jnp.bfloat16)
    outgoing = jnp.dot(
        placing_rows,
        jnp.concatenate([queries, tag], axis=1),
        preferred_element_type=jnp.float32,
    ).astype(jnp.bfloat16)
    landed = lax.all_to_all(outgoing, "dp", split_axis=0, concat_axis=0, tiled=True)
    arrived = landed[:, :columns]
    arrived_parent = landed[:, columns].astype(jnp.int32) - 1
    answered = jnp.zeros((slot_count, columns), jnp.bfloat16)
    for parent in range(parents_here):
        answer = attend(
            arrived, cached_key_rows[parent], cached_value_rows[parent], lengths[parent], kv_heads
        )
        answered = jnp.where((arrived_parent == parent)[:, None], answer, answered)
    partial_value = jnp.dot(answered, out_weight, preferred_element_type=jnp.float32)
    mine = lax.axis_index("tensor")
    blocks = partial_value.astype(jnp.bfloat16)
    summed = lax.dynamic_slice_in_dim(blocks, mine * half, half, 1).astype(jnp.float32)
    for step in range(1, tensor_count):
        target = lax.rem(mine + step, tensor_count)
        sent = lax.dynamic_slice_in_dim(blocks, target * half, half, 1)
        ring = [(i, (i + step) % tensor_count) for i in range(tensor_count)]
        summed = summed + lax.ppermute(sent, "tensor", ring).astype(jnp.float32)
    returned = lax.all_to_all(
        summed.astype(jnp.bfloat16), "dp", split_axis=0, concat_axis=0, tiled=True
    )
    mixed = lax.dot_general(
        placing_rows, returned, (((0,), (0,)), ((), ())), preferred_element_type=jnp.float32
    )
    return (residual.astype(jnp.float32) + mixed).astype(jnp.bfloat16)


def solution(mesh):
    placed = (
        P("dp", "tensor"),
        P("dp", None, "tensor"),
        P("dp", None, "tensor"),
        P("dp"),
        P("dp"),
        P("dp", "tensor"),
        P("tensor", None),
    )
    return jax.shard_map(
        local, mesh=mesh, in_specs=placed, out_specs=P("dp", "tensor"), check_vma=False
    )
```

```python
import functools
import math

import jax
import jax.numpy as jnp
from jax import lax
from jax.experimental import pallas as pl
from jax.experimental.pallas import tpu as pltpu
from jax.sharding import PartitionSpec as P

HEAD_WIDTH = 128


def attend(rows, key_block, value_block, prefix_length, kv_heads):
    slot_total, columns = rows.shape
    group_width = columns // (kv_heads * HEAD_WIDTH)
    prefix_span = key_block.shape[0]
    query_head_count = rows.reshape(slot_total, kv_heads, group_width, HEAD_WIDTH)
    key_heads = key_block.reshape(prefix_span, kv_heads, HEAD_WIDTH)
    value_heads = value_block.reshape(prefix_span, kv_heads, HEAD_WIDTH)
    scores = jnp.einsum(
        "sjgd,ljd->jsgl", query_head_count, key_heads, preferred_element_type=jnp.float32
    )
    scores = scores * (1.0 / math.sqrt(HEAD_WIDTH))
    live_mask = jnp.arange(prefix_span, dtype=jnp.int32) < prefix_length
    raised = jnp.where(live_mask, jnp.exp(scores), jnp.zeros((), jnp.float32))
    totals = jnp.sum(raised, axis=-1)
    summed = jnp.einsum(
        "jsgl,ljd->sjgd",
        raised.astype(jnp.bfloat16),
        value_heads,
        preferred_element_type=jnp.float32,
    )
    scaled = summed / jnp.transpose(totals, (1, 0, 2))[..., None]
    return scaled.reshape(slot_total, columns).astype(jnp.bfloat16)

PLANE = 4
MESH = pl.DeviceIdType.MESH
VMEM_MB = 40


SENDS = [(0, 0, 0), (0, 0, 1), (0, 0, 2), (0, 0, 3), (1, 1, 0), (1, 1, 1), (1, 1, 2), (1, 1, 3), (2, 2, 0), (2, 2, 1), (2, 2, 2), (2, 2, 3), (3, 3, 0), (3, 3, 1), (3, 3, 2), (3, 3, 3)]
STEP_OUTER, STEP_INNER = (0, 1, 3, 2), (0, 1, 2, 3)


def pick(outer, inner, at_inner, step):
    return sum(
        (o + at_inner * (i - o)) * jnp.where(step == k, 1, 0)
        for k, (o, i) in enumerate(zip(outer, inner))
    )


def flip(number, mask, bits):
    total = 0
    for bit in range(bits):
        unit = 1 << bit
        total = total + ((number // unit) % 2 + (mask // unit) % 2) % 2 * unit
    return total


def exchange_kernel(
    n, query_hbm, key_hbm, value_hbm, id_hbm, length_hbm, weight_hbm, mixed_ref,
    queries, keys, values, weight, lengths, ids, outgoing, landed, result, back,
    part_out, part_in, take, fetch_sem, id_send, id_recv, send_sem, recv_sem,
    part_send, part_recv, back_send, back_recv,
):
    me = lax.axis_index("dp")
    core = lax.axis_index("tensor")
    partner = 1 - core
    planes = n // PLANE
    bits = planes.bit_length() - 1
    my_plane, my_seat = me // PLANE, me % PLANE
    children, columns = queries.shape
    capacity = outgoing.shape[1]
    parents, span, _ = keys.shape
    kv_heads = keys.shape[2] // HEAD_WIDTH
    half = result.shape[2]
    group = columns // (kv_heads * HEAD_WIDTH)
    rows = PLANE * capacity
    slots = n * capacity

    fetches = [
        pltpu.make_async_copy(source, target, fetch_sem.at[i])
        for i, (source, target) in enumerate(
            [
                (id_hbm, ids.at[me]),
                (query_hbm, queries),
                (length_hbm, lengths),
                (key_hbm, keys),
                (value_hbm, values),
                (weight_hbm, weight),
            ]
        )
    ]
    for fetch in fetches[:2]:
        fetch.start()

    barrier = pltpu.get_barrier_semaphore()
    for step in range(1, n):
        pl.semaphore_signal(
            barrier, inc=1, device_id=((me + step) % n, core), device_id_type=MESH
        )
    pl.semaphore_signal(barrier, inc=1, device_id=(me, partner), device_id_type=MESH)
    def id_copy(target, slot):
        return pltpu.make_async_remote_copy(
            src_ref=ids.at[me],
            dst_ref=ids.at[slot],
            send_sem=id_send.at[target],
            recv_sem=id_recv.at[slot],
            device_id=(target, core),
            device_id_type=MESH,
        )

    def query_copy(target, slot):
        return pltpu.make_async_remote_copy(
            src_ref=outgoing.at[target],
            dst_ref=landed.at[slot],
            send_sem=send_sem.at[target],
            recv_sem=recv_sem.at[slot],
            device_id=(target, core),
            device_id_type=MESH,
        )

    def back_copy(target, slot):
        return pltpu.make_async_remote_copy(
            src_ref=result.at[target],
            dst_ref=back.at[slot],
            send_sem=back_send.at[target],
            recv_sem=back_recv.at[slot],
            device_id=(target, core),
            device_id_type=MESH,
        )

    def part_copy(g):
        return pltpu.make_async_remote_copy(
            src_ref=part_out.at[g],
            dst_ref=part_in.at[g],
            send_sem=part_send.at[g],
            recv_sem=part_recv.at[g],
            device_id=(me, partner),
            device_id_type=MESH,
        )

    fetches[0].wait()
    square = (children, children)
    across = jnp.broadcast_to(ids[me].astype(jnp.float32), square)
    down = across.T
    owner_across = jnp.floor((across + 0.5) * (1.0 / parents))
    owner_down = jnp.floor((down + 0.5) * (1.0 / parents))
    row_at = lax.broadcasted_iota(jnp.int32, square, 0)
    column_at = lax.broadcasted_iota(jnp.int32, square, 1)
    zero, one = jnp.zeros(square, jnp.float32), jnp.ones(square, jnp.float32)
    kin = owner_across == owner_down
    alike = jnp.where(across == down, one, zero)
    lower = jnp.where(column_at < row_at, alike, zero)
    upper = jnp.where(row_at < column_at, alike, zero)
    before_down = jnp.where(kin, jnp.where(across < down, one, lower), zero)
    before_across = jnp.where(kin, jnp.where(down < across, one, upper), zero)
    slot_down = owner_down[:, :1] * capacity + jnp.sum(before_down, axis=1, keepdims=True)
    slot_across = owner_across[:1] * capacity + jnp.sum(before_across, axis=0, keepdims=True)
    place = jnp.where(
        lax.broadcasted_iota(jnp.int32, (slots, children), 0).astype(jnp.float32) == slot_across,
        jnp.ones((slots, children), jnp.float32),
        jnp.zeros((slots, children), jnp.float32),
    ).astype(jnp.bfloat16)
    fetches[1].wait()
    for fetch in fetches[2:]:
        fetch.start()
    outgoing[...] = (
        jnp.dot(place, queries[...], preferred_element_type=jnp.float32)
        .astype(jnp.bfloat16)
        .reshape(n, capacity, columns)
    )
    pl.semaphore_wait(barrier, n)

    for step in range(1, n):
        id_copy((me + step) % n, me).start()
    at_inner = (my_plane + 1) // 2 % 2
    for o, inner, i in SENDS:
        mask = o + at_inner * (inner - o)
        target = flip(my_plane, mask, bits) * PLANE + flip(my_seat, i, 2)
        if i == 0 and 0 in (o, inner):

            @pl.when(mask > 0)
            def _(target=target):
                query_copy(target, me).start()
        else:
            query_copy(target, me).start()
    take[...] = jnp.where(
        lax.broadcasted_iota(jnp.int32, (children, slots), 1).astype(jnp.float32) == slot_down,
        jnp.ones((children, slots), jnp.float32),
        jnp.zeros((children, slots), jnp.float32),
    ).astype(jnp.bfloat16)
    landed[me] = outgoing[me]
    for fetch in fetches[2:]:
        fetch.wait()
    for step in range(1, n):
        other = (me + step) % n
        id_copy(other, other).wait_recv()
    scale = math.log2(math.e) / math.sqrt(HEAD_WIDTH)

    @pl.loop(0, planes)
    def _(g):
        mask = pick(STEP_OUTER, STEP_INNER, at_inner, g)
        plane = flip(my_plane, mask, bits)
        seats = [plane * PLANE + flip(my_seat, i, 2) for i in range(PLANE)]

        @pl.when(mask > 0)
        def _():
            query_copy(seats[0], seats[0]).wait_recv()

        for i in range(1, PLANE):
            query_copy(seats[i], seats[i]).wait_recv()

        base = plane * PLANE
        spot = lax.broadcasted_iota(jnp.int32, (capacity, 1), 0).astype(jnp.float32)
        tag_parts = []
        for i in range(PLANE):
            known = ids[base + i]
            number = jnp.zeros((capacity, 1), jnp.float32)
            for p in range(parents - 1):
                smaller = jnp.where(
                    known >= me * parents, jnp.where(known <= me * parents + p, 1.0, 0.0), 0.0
                )
                count = jnp.sum(smaller, axis=1, keepdims=True)
                number = number + jnp.where(spot >= count, 1.0, 0.0)
            tag_parts.append(number)
        tags = jnp.concatenate(tag_parts * group, axis=0)
        belongs = [tags == float(p) for p in range(parents)]
        limit = jnp.full(tags.shape, lengths[parents - 1], jnp.int32)
        for p in range(parents - 1):
            limit = jnp.where(belongs[p], lengths[p], limit)
        live = lax.broadcasted_iota(jnp.int32, (rows * group, span), 1) < limit
        pieces = []
        for j in range(kv_heads):
            at = j * HEAD_WIDTH
            q = jnp.concatenate(
                [
                    landed[
                        pl.ds(base, PLANE), :, (j * group + h) * HEAD_WIDTH:(j * group + h + 1) * HEAD_WIDTH
                    ].reshape(rows, HEAD_WIDTH)
                    for h in range(group)
                ],
                axis=0,
            )
            spread = jnp.concatenate(
                [jnp.where(belongs[p], q, jnp.zeros_like(q)) for p in range(parents)], axis=1
            )
            key_pair = jnp.concatenate(
                [keys[p, :, at:at + HEAD_WIDTH] for p in range(parents)], axis=1
            )
            scores = lax.dot_general(
                spread, key_pair, (((1,), (1,)), ((), ())), preferred_element_type=jnp.float32
            )
            raised = jnp.where(live, jnp.exp2(scores * scale), 0.0)
            totals = jnp.sum(raised, axis=1, keepdims=True)
            soft = raised.astype(jnp.bfloat16)
            value_pair = jnp.concatenate(
                [values[p, :, at:at + HEAD_WIDTH] for p in range(parents)], axis=1
            )
            both = jnp.dot(soft, value_pair, preferred_element_type=jnp.float32)
            summed = both[:, (parents - 1) * HEAD_WIDTH:]
            for p in range(parents - 1):
                summed = jnp.where(
                    belongs[p], both[:, p * HEAD_WIDTH:(p + 1) * HEAD_WIDTH], summed
                )
            answer = (summed / totals).astype(jnp.bfloat16)
            pieces += [answer[h * rows:(h + 1) * rows] for h in range(group)]
        attended = jnp.concatenate(pieces, axis=1)
        theirs = pl.multiple_of(partner * half, HEAD_WIDTH)
        mine = pl.multiple_of(core * half, HEAD_WIDTH)
        part_out[g] = jnp.dot(
            attended, weight[:, pl.ds(theirs, half)], preferred_element_type=jnp.float32
        ).astype(jnp.bfloat16)
        part_copy(g).start()
        own = jnp.dot(
            attended, weight[:, pl.ds(mine, half)], preferred_element_type=jnp.float32
        )
        part_copy(g).wait_recv()
        total = (own + part_in[g].astype(jnp.float32)).astype(jnp.bfloat16)
        result[pl.ds(base, PLANE)] = total.reshape(PLANE, capacity, half)

        @pl.when(mask > 0)
        def _():
            back_copy(seats[0], me).start()

        for i in range(1, PLANE):
            back_copy(seats[i], me).start()

    back[me] = result[me]
    for step in range(1, n):
        other = (me + step) % n
        back_copy(other, other).wait_recv()
    mixed = jnp.dot(
        take[...], back[...].reshape(slots, half), preferred_element_type=jnp.float32
    )
    mixed_ref[...] = mixed.astype(jnp.bfloat16)
    for step in range(1, n):
        other = (me + step) % n
        id_copy(other, me).wait_send()
        query_copy(other, me).wait_send()
        back_copy(other, me).wait_send()
    for g in range(planes):
        part_copy(g).wait_send()


def exchange(n, capacity, queries, cached_key_rows, cached_value_rows, parent_ids, lengths, residual, out_weight):
    children, columns = queries.shape
    half = residual.shape[1]
    planes = n // PLANE
    anywhere = pl.BlockSpec(memory_space=pltpu.HBM)
    rows = PLANE * capacity
    dma = pltpu.SemaphoreType.DMA

    def held(*shape):
        return pltpu.VMEM(shape, jnp.bfloat16)

    return pl.pallas_call(
        functools.partial(exchange_kernel, n),
        out_shape=jax.ShapeDtypeStruct(residual.shape, jnp.bfloat16),
        in_specs=[anywhere] * 6,
        out_specs=pl.BlockSpec(memory_space=pltpu.VMEM),
        scratch_shapes=[
            held(*queries.shape),
            held(*cached_key_rows.shape),
            held(*cached_value_rows.shape),
            held(*out_weight.shape),
            pltpu.SMEM(lengths.shape, jnp.int32),
            pltpu.VMEM((n, 1, children), jnp.int32),
            held(n, capacity, columns),
            held(n, capacity, columns),
            held(n, capacity, half),
            held(n, capacity, half),
            held(planes, rows, half),
            held(planes, rows, half),
            held(children, n * capacity),
            dma((6,)), dma((n,)), dma((n,)), dma((n,)), dma((n,)),
            dma((planes,)), dma((planes,)), dma((n,)), dma((n,)),
        ],
        compiler_params=pltpu.CompilerParams(
            collective_id=0, has_side_effects=True, vmem_limit_bytes=VMEM_MB << 20
        ),
    )(
        *(
            pltpu.with_memory_space_constraint(operand, pltpu.HBM)
            for operand in (
                queries,
                cached_key_rows,
                cached_value_rows,
                parent_ids.reshape(1, children),
                lengths,
                out_weight,
            )
        )
    )


def local(queries, cached_key_rows, cached_value_rows, parent_ids, lengths, residual, out_weight):
    dp_count = lax.axis_size("dp")
    children = queries.shape[0]
    columns = queries.shape[1]
    kv_heads = cached_key_rows.shape[2] // HEAD_WIDTH
    parents_here = lengths.shape[0]
    capacity = max(2, 2 * children // dp_count)
    half = residual.shape[1]
    tensor_count = lax.axis_size("tensor")
    planes = dp_count // PLANE
    if (
        capacity % 16 == 0
        and children % 128 == 0
        and dp_count % PLANE == 0
        and planes & (planes - 1) == 0
        and tensor_count == 2
    ):
        mixed = exchange(
            dp_count, capacity, queries, cached_key_rows, cached_value_rows, parent_ids, lengths, residual, out_weight
        )
        return (residual.astype(jnp.float32) + mixed.astype(jnp.float32)).astype(jnp.bfloat16)
    owner_of = parent_ids // parents_here
    sub_index = parent_ids % parents_here
    slot_count = dp_count * capacity
    order_rows = jnp.arange(children, dtype=jnp.int32)
    earlier = (owner_of[:, None] == owner_of[None, :]) & (order_rows[:, None] > order_rows[None, :])
    slot_rank = jnp.sum(earlier.astype(jnp.int32), axis=1)
    slot_of = owner_of * capacity + slot_rank
    placing = jnp.arange(slot_count, dtype=jnp.int32)[:, None] == slot_of[None, :]
    placing_rows = placing.astype(jnp.bfloat16)
    tag = jnp.broadcast_to((sub_index + 1)[:, None], (children, HEAD_WIDTH)).astype(jnp.bfloat16)
    outgoing = jnp.dot(
        placing_rows,
        jnp.concatenate([queries, tag], axis=1),
        preferred_element_type=jnp.float32,
    ).astype(jnp.bfloat16)
    landed = lax.all_to_all(outgoing, "dp", split_axis=0, concat_axis=0, tiled=True)
    arrived = landed[:, :columns]
    arrived_parent = landed[:, columns].astype(jnp.int32) - 1
    answered = jnp.zeros((slot_count, columns), jnp.bfloat16)
    for parent in range(parents_here):
        answer = attend(
            arrived, cached_key_rows[parent], cached_value_rows[parent], lengths[parent], kv_heads
        )
        answered = jnp.where((arrived_parent == parent)[:, None], answer, answered)
    partial_value = jnp.dot(answered, out_weight, preferred_element_type=jnp.float32)
    mine = lax.axis_index("tensor")
    blocks = partial_value.astype(jnp.bfloat16)
    summed = lax.dynamic_slice_in_dim(blocks, mine * half, half, 1).astype(jnp.float32)
    for step in range(1, tensor_count):
        target = lax.rem(mine + step, tensor_count)
        sent = lax.dynamic_slice_in_dim(blocks, target * half, half, 1)
        ring = [(i, (i + step) % tensor_count) for i in range(tensor_count)]
        summed = summed + lax.ppermute(sent, "tensor", ring).astype(jnp.float32)
    returned = lax.all_to_all(
        summed.astype(jnp.bfloat16), "dp", split_axis=0, concat_axis=0, tiled=True
    )
    mixed = lax.dot_general(
        placing_rows, returned, (((0,), (0,)), ((), ())), preferred_element_type=jnp.float32
    )
    return (residual.astype(jnp.float32) + mixed).astype(jnp.bfloat16)


def solution(mesh):
    placed = (
        P("dp", "tensor"),
        P("dp", None, "tensor"),
        P("dp", None, "tensor"),
        P("dp"),
        P("dp"),
        P("dp", "tensor"),
        P("tensor", None),
    )
    return jax.shard_map(
        local, mesh=mesh, in_specs=placed, out_specs=P("dp", "tensor"), check_vma=False
    )
```

```python
import functools
import math

import jax
import jax.numpy as jnp
from jax import lax
from jax.experimental import pallas as pl
from jax.experimental.pallas import tpu as pltpu
from jax.sharding import PartitionSpec as P

HEAD_WIDTH = 128


def attend(rows, key_block, value_block, prefix_length, kv_heads):
    slot_total, columns = rows.shape
    group_width = columns // (kv_heads * HEAD_WIDTH)
    prefix_span = key_block.shape[0]
    query_head_count = rows.reshape(slot_total, kv_heads, group_width, HEAD_WIDTH)
    key_heads = key_block.reshape(prefix_span, kv_heads, HEAD_WIDTH)
    value_heads = value_block.reshape(prefix_span, kv_heads, HEAD_WIDTH)
    scores = jnp.einsum(
        "sjgd,ljd->jsgl", query_head_count, key_heads, preferred_element_type=jnp.float32
    )
    scores = scores * (1.0 / math.sqrt(HEAD_WIDTH))
    live_mask = jnp.arange(prefix_span, dtype=jnp.int32) < prefix_length
    raised = jnp.where(live_mask, jnp.exp(scores), jnp.zeros((), jnp.float32))
    totals = jnp.sum(raised, axis=-1)
    summed = jnp.einsum(
        "jsgl,ljd->sjgd",
        raised.astype(jnp.bfloat16),
        value_heads,
        preferred_element_type=jnp.float32,
    )
    scaled = summed / jnp.transpose(totals, (1, 0, 2))[..., None]
    return scaled.reshape(slot_total, columns).astype(jnp.bfloat16)

PLANE = 4
MESH = pl.DeviceIdType.MESH
VMEM_MB = 40


FIRST, SECOND, OUTER = (0, 3), (1, 2), (0, 1, 2, 3)
STEP_OUTER, STEP_INNER = (0, 1, 3, 2), (0, 1, 2, 3)


def pick(outer, inner, at_inner, step):
    return sum(
        (o + at_inner * (i - o)) * jnp.where(step == k, 1, 0)
        for k, (o, i) in enumerate(zip(outer, inner))
    )


def flip(number, mask, bits):
    total = 0
    for bit in range(bits):
        unit = 1 << bit
        total = total + ((number // unit) % 2 + (mask // unit) % 2) % 2 * unit
    return total


def exchange_kernel(
    n, query_hbm, key_hbm, value_hbm, id_hbm, length_hbm, weight_hbm, mixed_ref,
    queries, keys, values, weight, lengths, ids, outgoing, landed, result, back,
    part_out, part_in, own, take, fetch_sem, id_send, id_recv, send_sem, recv_sem,
    part_send, part_recv, back_send, back_recv,
):
    me = lax.axis_index("dp")
    core = lax.axis_index("tensor")
    partner = 1 - core
    planes = n // PLANE
    bits = planes.bit_length() - 1
    my_plane, my_seat = me // PLANE, me % PLANE
    children, columns = queries.shape
    capacity = outgoing.shape[1]
    parents, span, _ = keys.shape
    kv_heads = keys.shape[2] // HEAD_WIDTH
    half = result.shape[2]
    group = columns // (kv_heads * HEAD_WIDTH)
    rows = PLANE * capacity
    slots = n * capacity

    fetches = [
        pltpu.make_async_copy(source, target, fetch_sem.at[i])
        for i, (source, target) in enumerate(
            [
                (id_hbm, ids.at[me]),
                (query_hbm, queries),
                (length_hbm, lengths),
                (key_hbm, keys),
                (value_hbm, values),
                (weight_hbm, weight),
            ]
        )
    ]
    for fetch in fetches[:2]:
        fetch.start()

    barrier = pltpu.get_barrier_semaphore()
    at_inner = (my_plane + 1) // 2 % 2

    def greet(mask):
        for i in range(PLANE):
            target = flip(my_plane, mask, bits) * PLANE + flip(my_seat, i, 2)
            if mask or i:
                pl.semaphore_signal(barrier, inc=1, device_id=(target, core), device_id_type=MESH)

    for mask in FIRST:
        greet(mask)
    pl.semaphore_signal(barrier, inc=1, device_id=(me, partner), device_id_type=MESH)
    def id_copy(target, slot):
        return pltpu.make_async_remote_copy(
            src_ref=ids.at[me],
            dst_ref=ids.at[slot],
            send_sem=id_send.at[target],
            recv_sem=id_recv.at[slot],
            device_id=(target, core),
            device_id_type=MESH,
        )

    def query_copy(target, slot):
        return pltpu.make_async_remote_copy(
            src_ref=outgoing.at[target],
            dst_ref=landed.at[slot],
            send_sem=send_sem.at[target],
            recv_sem=recv_sem.at[slot],
            device_id=(target, core),
            device_id_type=MESH,
        )

    def back_copy(target, slot):
        return pltpu.make_async_remote_copy(
            src_ref=result.at[target],
            dst_ref=back.at[slot],
            send_sem=back_send.at[target],
            recv_sem=back_recv.at[slot],
            device_id=(target, core),
            device_id_type=MESH,
        )

    def part_copy(g):
        return pltpu.make_async_remote_copy(
            src_ref=part_out.at[g],
            dst_ref=part_in.at[g],
            send_sem=part_send.at[g],
            recv_sem=part_recv.at[g],
            device_id=(me, partner),
            device_id_type=MESH,
        )

    fetches[0].wait()
    square = (children, children)
    across = jnp.broadcast_to(ids[me].astype(jnp.float32), square)
    down = across.T
    owner_across = jnp.floor((across + 0.5) * (1.0 / parents))
    owner_down = jnp.floor((down + 0.5) * (1.0 / parents))
    row_at = lax.broadcasted_iota(jnp.int32, square, 0)
    column_at = lax.broadcasted_iota(jnp.int32, square, 1)
    zero, one = jnp.zeros(square, jnp.float32), jnp.ones(square, jnp.float32)
    kin = owner_across == owner_down
    alike = jnp.where(across == down, one, zero)
    lower = jnp.where(column_at < row_at, alike, zero)
    upper = jnp.where(row_at < column_at, alike, zero)
    before_down = jnp.where(kin, jnp.where(across < down, one, lower), zero)
    before_across = jnp.where(kin, jnp.where(down < across, one, upper), zero)
    slot_down = owner_down[:, :1] * capacity + jnp.sum(before_down, axis=1, keepdims=True)
    slot_across = owner_across[:1] * capacity + jnp.sum(before_across, axis=0, keepdims=True)
    place = jnp.where(
        lax.broadcasted_iota(jnp.int32, (slots, children), 0).astype(jnp.float32) == slot_across,
        jnp.ones((slots, children), jnp.float32),
        jnp.zeros((slots, children), jnp.float32),
    ).astype(jnp.bfloat16)
    fetches[1].wait()
    for fetch in fetches[2:]:
        fetch.start()
    outgoing[...] = (
        jnp.dot(place, queries[...], preferred_element_type=jnp.float32)
        .astype(jnp.bfloat16)
        .reshape(n, capacity, columns)
    )
    def send(masks):
        for mask in masks:
            for i in range(PLANE):
                target = flip(my_plane, mask, bits) * PLANE + flip(my_seat, i, 2)
                if mask or i:
                    id_copy(target, me).start()
        for mask in masks:
            for i in range(PLANE):
                target = flip(my_plane, mask, bits) * PLANE + flip(my_seat, i, 2)
                if mask or i:
                    query_copy(target, me).start()

    @pl.when(at_inner == 1)
    def _():
        pl.semaphore_wait(barrier, n // 2)
        for mask in SECOND:
            greet(mask)
        send(FIRST)
        pl.semaphore_wait(barrier, n // 2)
        send(SECOND)

    @pl.when(at_inner == 0)
    def _():
        pl.semaphore_wait(barrier, n)
        for mask in SECOND:
            greet(mask)
        send(OUTER)

    take[...] = jnp.where(
        lax.broadcasted_iota(jnp.int32, (children, slots), 1).astype(jnp.float32) == slot_down,
        jnp.ones((children, slots), jnp.float32),
        jnp.zeros((children, slots), jnp.float32),
    ).astype(jnp.bfloat16)
    landed[me] = outgoing[me]
    for fetch in fetches[2:]:
        fetch.wait()
    for step in range(1, n):
        other = (me + step) % n
        id_copy(other, other).wait_recv()
    scale = math.log2(math.e) / math.sqrt(HEAD_WIDTH)

    @pl.loop(0, planes)
    def _(g):
        mask = pick(STEP_OUTER, STEP_INNER, at_inner, g)
        plane = flip(my_plane, mask, bits)
        seats = [plane * PLANE + flip(my_seat, i, 2) for i in range(PLANE)]

        @pl.when(mask > 0)
        def _():
            query_copy(seats[0], seats[0]).wait_recv()

        for i in range(1, PLANE):
            query_copy(seats[i], seats[i]).wait_recv()

        base = plane * PLANE
        spot = lax.broadcasted_iota(jnp.int32, (capacity, 1), 0).astype(jnp.float32)
        tag_parts = []
        for i in range(PLANE):
            known = ids[base + i]
            number = jnp.zeros((capacity, 1), jnp.float32)
            for p in range(parents - 1):
                smaller = jnp.where(
                    known >= me * parents, jnp.where(known <= me * parents + p, 1.0, 0.0), 0.0
                )
                count = jnp.sum(smaller, axis=1, keepdims=True)
                number = number + jnp.where(spot >= count, 1.0, 0.0)
            tag_parts.append(number)
        tags = jnp.concatenate(tag_parts * group, axis=0)
        belongs = [tags == float(p) for p in range(parents)]
        limit = jnp.full(tags.shape, lengths[parents - 1], jnp.int32)
        for p in range(parents - 1):
            limit = jnp.where(belongs[p], lengths[p], limit)
        live = lax.broadcasted_iota(jnp.int32, (rows * group, span), 1) < limit
        pieces = []
        for j in range(kv_heads):
            at = j * HEAD_WIDTH
            q = jnp.concatenate(
                [
                    landed[
                        pl.ds(base, PLANE), :, (j * group + h) * HEAD_WIDTH:(j * group + h + 1) * HEAD_WIDTH
                    ].reshape(rows, HEAD_WIDTH)
                    for h in range(group)
                ],
                axis=0,
            )
            spread = jnp.concatenate(
                [jnp.where(belongs[p], q, jnp.zeros_like(q)) for p in range(parents)], axis=1
            )
            key_pair = jnp.concatenate(
                [keys[p, :, at:at + HEAD_WIDTH] for p in range(parents)], axis=1
            )
            scores = lax.dot_general(
                spread, key_pair, (((1,), (1,)), ((), ())), preferred_element_type=jnp.float32
            )
            raised = jnp.where(live, jnp.exp2(scores * scale), 0.0)
            totals = jnp.sum(raised, axis=1, keepdims=True)
            soft = raised.astype(jnp.bfloat16)
            value_pair = jnp.concatenate(
                [values[p, :, at:at + HEAD_WIDTH] for p in range(parents)], axis=1
            )
            both = jnp.dot(soft, value_pair, preferred_element_type=jnp.float32)
            summed = both[:, (parents - 1) * HEAD_WIDTH:]
            for p in range(parents - 1):
                summed = jnp.where(
                    belongs[p], both[:, p * HEAD_WIDTH:(p + 1) * HEAD_WIDTH], summed
                )
            answer = (summed / totals).astype(jnp.bfloat16)
            pieces += [answer[h * rows:(h + 1) * rows] for h in range(group)]
        attended = jnp.concatenate(pieces, axis=1)
        theirs = pl.multiple_of(partner * half, HEAD_WIDTH)
        mine = pl.multiple_of(core * half, HEAD_WIDTH)
        part_out[g] = jnp.dot(
            attended, weight[:, pl.ds(theirs, half)], preferred_element_type=jnp.float32
        ).astype(jnp.bfloat16)
        part_copy(g).start()
        own[...] = jnp.dot(
            attended, weight[:, pl.ds(mine, half)], preferred_element_type=jnp.float32
        )
        part_copy(g).wait_recv()
        total = (own[...] + part_in[g].astype(jnp.float32)).astype(jnp.bfloat16)
        result[pl.ds(base, PLANE)] = total.reshape(PLANE, capacity, half)

        @pl.when(mask > 0)
        def _():
            back_copy(seats[0], me).start()

        for i in range(1, PLANE):
            back_copy(seats[i], me).start()

    back[me] = result[me]
    for step in range(1, n):
        other = (me + step) % n
        id_copy(other, me).wait_send()
        query_copy(other, me).wait_send()
    for g in range(planes):
        part_copy(g).wait_send()
    for step in range(1, n):
        other = (me + step) % n
        back_copy(other, other).wait_recv()
    mixed = jnp.dot(
        take[...], back[...].reshape(slots, half), preferred_element_type=jnp.float32
    )
    mixed_ref[...] = mixed.astype(jnp.bfloat16)
    for step in range(1, n):
        back_copy((me + step) % n, me).wait_send()


def exchange(n, capacity, queries, cached_key_rows, cached_value_rows, parent_ids, lengths, residual, out_weight):
    children, columns = queries.shape
    half = residual.shape[1]
    planes = n // PLANE
    anywhere = pl.BlockSpec(memory_space=pltpu.HBM)
    rows = PLANE * capacity
    dma = pltpu.SemaphoreType.DMA

    def held(*shape):
        return pltpu.VMEM(shape, jnp.bfloat16)

    return pl.pallas_call(
        functools.partial(exchange_kernel, n),
        out_shape=jax.ShapeDtypeStruct(residual.shape, jnp.bfloat16),
        in_specs=[anywhere] * 6,
        out_specs=pl.BlockSpec(memory_space=pltpu.VMEM),
        scratch_shapes=[
            held(*queries.shape),
            held(*cached_key_rows.shape),
            held(*cached_value_rows.shape),
            held(*out_weight.shape),
            pltpu.SMEM(lengths.shape, jnp.int32),
            pltpu.VMEM((n, 1, children), jnp.int32),
            held(n, capacity, columns),
            held(n, capacity, columns),
            held(n, capacity, half),
            held(n, capacity, half),
            held(planes, rows, half),
            held(planes, rows, half),
            pltpu.VMEM((rows, half), jnp.float32),
            held(children, n * capacity),
            dma((6,)), dma((n,)), dma((n,)), dma((n,)), dma((n,)),
            dma((planes,)), dma((planes,)), dma((n,)), dma((n,)),
        ],
        compiler_params=pltpu.CompilerParams(
            collective_id=0, has_side_effects=True, vmem_limit_bytes=VMEM_MB << 20
        ),
    )(
        *(
            pltpu.with_memory_space_constraint(operand, pltpu.HBM)
            for operand in (
                queries,
                cached_key_rows,
                cached_value_rows,
                parent_ids.reshape(1, children),
                lengths,
                out_weight,
            )
        )
    )


def local(queries, cached_key_rows, cached_value_rows, parent_ids, lengths, residual, out_weight):
    dp_count = lax.axis_size("dp")
    children = queries.shape[0]
    columns = queries.shape[1]
    kv_heads = cached_key_rows.shape[2] // HEAD_WIDTH
    parents_here = lengths.shape[0]
    capacity = max(2, 2 * children // dp_count)
    half = residual.shape[1]
    tensor_count = lax.axis_size("tensor")
    planes = dp_count // PLANE
    if (
        capacity % 16 == 0
        and children % 128 == 0
        and dp_count % PLANE == 0
        and planes == len(SECOND + FIRST)
        and tensor_count == 2
    ):
        mixed = exchange(
            dp_count, capacity, queries, cached_key_rows, cached_value_rows, parent_ids, lengths, residual, out_weight
        )
        return (residual.astype(jnp.float32) + mixed.astype(jnp.float32)).astype(jnp.bfloat16)
    owner_of = parent_ids // parents_here
    sub_index = parent_ids % parents_here
    slot_count = dp_count * capacity
    order_rows = jnp.arange(children, dtype=jnp.int32)
    earlier = (owner_of[:, None] == owner_of[None, :]) & (order_rows[:, None] > order_rows[None, :])
    slot_rank = jnp.sum(earlier.astype(jnp.int32), axis=1)
    slot_of = owner_of * capacity + slot_rank
    placing = jnp.arange(slot_count, dtype=jnp.int32)[:, None] == slot_of[None, :]
    placing_rows = placing.astype(jnp.bfloat16)
    tag = jnp.broadcast_to((sub_index + 1)[:, None], (children, HEAD_WIDTH)).astype(jnp.bfloat16)
    outgoing = jnp.dot(
        placing_rows,
        jnp.concatenate([queries, tag], axis=1),
        preferred_element_type=jnp.float32,
    ).astype(jnp.bfloat16)
    landed = lax.all_to_all(outgoing, "dp", split_axis=0, concat_axis=0, tiled=True)
    arrived = landed[:, :columns]
    arrived_parent = landed[:, columns].astype(jnp.int32) - 1
    answered = jnp.zeros((slot_count, columns), jnp.bfloat16)
    for parent in range(parents_here):
        answer = attend(
            arrived, cached_key_rows[parent], cached_value_rows[parent], lengths[parent], kv_heads
        )
        answered = jnp.where((arrived_parent == parent)[:, None], answer, answered)
    partial_value = jnp.dot(answered, out_weight, preferred_element_type=jnp.float32)
    mine = lax.axis_index("tensor")
    blocks = partial_value.astype(jnp.bfloat16)
    summed = lax.dynamic_slice_in_dim(blocks, mine * half, half, 1).astype(jnp.float32)
    for step in range(1, tensor_count):
        target = lax.rem(mine + step, tensor_count)
        sent = lax.dynamic_slice_in_dim(blocks, target * half, half, 1)
        ring = [(i, (i + step) % tensor_count) for i in range(tensor_count)]
        summed = summed + lax.ppermute(sent, "tensor", ring).astype(jnp.float32)
    returned = lax.all_to_all(
        summed.astype(jnp.bfloat16), "dp", split_axis=0, concat_axis=0, tiled=True
    )
    mixed = lax.dot_general(
        placing_rows, returned, (((0,), (0,)), ((), ())), preferred_element_type=jnp.float32
    )
    return (residual.astype(jnp.float32) + mixed).astype(jnp.bfloat16)


def solution(mesh):
    placed = (
        P("dp", "tensor"),
        P("dp", None, "tensor"),
        P("dp", None, "tensor"),
        P("dp"),
        P("dp"),
        P("dp", "tensor"),
        P("tensor", None),
    )
    return jax.shard_map(
        local, mesh=mesh, in_specs=placed, out_specs=P("dp", "tensor"), check_vma=False
    )
```

```python
import functools
import math

import jax
import jax.numpy as jnp
from jax import lax
from jax.experimental import pallas as pl
from jax.experimental.pallas import tpu as pltpu
from jax.sharding import PartitionSpec as P

HEAD_WIDTH = 128


def attend(rows, key_block, value_block, prefix_length, kv_heads):
    slot_total, columns = rows.shape
    group_width = columns // (kv_heads * HEAD_WIDTH)
    prefix_span = key_block.shape[0]
    query_head_count = rows.reshape(slot_total, kv_heads, group_width, HEAD_WIDTH)
    key_heads = key_block.reshape(prefix_span, kv_heads, HEAD_WIDTH)
    value_heads = value_block.reshape(prefix_span, kv_heads, HEAD_WIDTH)
    scores = jnp.einsum(
        "sjgd,ljd->jsgl", query_head_count, key_heads, preferred_element_type=jnp.float32
    )
    scores = scores * (1.0 / math.sqrt(HEAD_WIDTH))
    live_mask = jnp.arange(prefix_span, dtype=jnp.int32) < prefix_length
    raised = jnp.where(live_mask, jnp.exp(scores), jnp.zeros((), jnp.float32))
    totals = jnp.sum(raised, axis=-1)
    summed = jnp.einsum(
        "jsgl,ljd->sjgd",
        raised.astype(jnp.bfloat16),
        value_heads,
        preferred_element_type=jnp.float32,
    )
    scaled = summed / jnp.transpose(totals, (1, 0, 2))[..., None]
    return scaled.reshape(slot_total, columns).astype(jnp.bfloat16)

PLANE = 4
MESH = pl.DeviceIdType.MESH
VMEM_MB = 40


FIRST, SECOND, OUTER = (0, 3), (1, 2), (0, 1, 2, 3)
STEP_OUTER, STEP_INNER = (0, 1, 3, 2), (0, 1, 2, 3)


def pick(outer, inner, at_inner, step):
    return sum(
        (o + at_inner * (i - o)) * jnp.where(step == k, 1, 0)
        for k, (o, i) in enumerate(zip(outer, inner))
    )


def flip(number, mask, bits):
    total = 0
    for bit in range(bits):
        unit = 1 << bit
        total = total + ((number // unit) % 2 + (mask // unit) % 2) % 2 * unit
    return total


def exchange_kernel(
    n, query_hbm, key_hbm, value_hbm, id_hbm, length_hbm, weight_hbm, mixed_ref,
    queries, keys, values, weight, lengths, ids, outgoing, landed, result, back,
    part_out, part_in, own, take, fetch_sem, id_send, id_recv, send_sem, recv_sem,
    part_send, part_recv, back_send, back_recv,
):
    me = lax.axis_index("dp")
    core = lax.axis_index("tensor")
    partner = 1 - core
    planes = n // PLANE
    bits = planes.bit_length() - 1
    my_plane, my_seat = me // PLANE, me % PLANE
    children, columns = queries.shape
    capacity = outgoing.shape[1]
    parents, span, _ = keys.shape
    kv_heads = keys.shape[2] // HEAD_WIDTH
    half = result.shape[2]
    group = columns // (kv_heads * HEAD_WIDTH)
    rows = PLANE * capacity
    slots = n * capacity

    fetches = [
        pltpu.make_async_copy(source, target, fetch_sem.at[i])
        for i, (source, target) in enumerate(
            [
                (id_hbm, ids.at[me]),
                (query_hbm, queries),
                (length_hbm, lengths),
                (key_hbm, keys),
                (value_hbm, values),
                (weight_hbm, weight),
            ]
        )
    ]
    for fetch in fetches[:2]:
        fetch.start()

    barrier = pltpu.get_barrier_semaphore()
    at_inner = (my_plane + 1) // 2 % 2

    def greet(mask):
        for i in range(PLANE):
            target = flip(my_plane, mask, bits) * PLANE + flip(my_seat, i, 2)
            if mask or i:
                pl.semaphore_signal(barrier, inc=1, device_id=(target, core), device_id_type=MESH)

    for mask in FIRST:
        greet(mask)
    pl.semaphore_signal(barrier, inc=1, device_id=(me, partner), device_id_type=MESH)
    def remote(source, target, send, recv, device):
        return pltpu.make_async_remote_copy(
            src_ref=source,
            dst_ref=target,
            send_sem=send,
            recv_sem=recv,
            device_id=device,
            device_id_type=MESH,
        )

    def id_copy(target):
        return remote(ids.at[me], ids.at[me], id_send, id_recv, (target, core))

    def query_copy(target, mask):
        return remote(
            outgoing.at[target], landed.at[me], send_sem, recv_sem.at[mask], (target, core)
        )

    def back_copy(target):
        return remote(result.at[target], back.at[me], back_send, back_recv, (target, core))

    def part_copy(g):
        return remote(
            part_out.at[g], part_in.at[g], part_send.at[g], part_recv.at[g], (me, partner)
        )

    def blocks(source, target, count, send, recv):
        return remote(
            source.at[pl.ds(0, count)], target.at[pl.ds(0, count)], send, recv, (me, partner)
        )

    fetches[0].wait()
    square = (children, children)
    across = jnp.broadcast_to(ids[me].astype(jnp.float32), square)
    down = across.T
    owner_across = jnp.floor((across + 0.5) * (1.0 / parents))
    owner_down = jnp.floor((down + 0.5) * (1.0 / parents))
    row_at = lax.broadcasted_iota(jnp.int32, square, 0)
    column_at = lax.broadcasted_iota(jnp.int32, square, 1)
    zero, one = jnp.zeros(square, jnp.float32), jnp.ones(square, jnp.float32)
    kin = owner_across == owner_down
    alike = jnp.where(across == down, one, zero)
    lower = jnp.where(column_at < row_at, alike, zero)
    upper = jnp.where(row_at < column_at, alike, zero)
    before_down = jnp.where(kin, jnp.where(across < down, one, lower), zero)
    before_across = jnp.where(kin, jnp.where(down < across, one, upper), zero)
    slot_down = owner_down[:, :1] * capacity + jnp.sum(before_down, axis=1, keepdims=True)
    slot_across = owner_across[:1] * capacity + jnp.sum(before_across, axis=0, keepdims=True)
    place = jnp.where(
        lax.broadcasted_iota(jnp.int32, (slots, children), 0).astype(jnp.float32) == slot_across,
        jnp.ones((slots, children), jnp.float32),
        jnp.zeros((slots, children), jnp.float32),
    ).astype(jnp.bfloat16)
    fetches[1].wait()
    for fetch in fetches[2:]:
        fetch.start()
    outgoing[...] = (
        jnp.dot(place, queries[...], preferred_element_type=jnp.float32)
        .astype(jnp.bfloat16)
        .reshape(n, capacity, columns)
    )
    def send(masks):
        for mask in masks:
            for i in range(PLANE):
                target = flip(my_plane, mask, bits) * PLANE + flip(my_seat, i, 2)
                if mask or i:
                    id_copy(target).start()
        for mask in masks:
            for i in range(PLANE):
                target = flip(my_plane, mask, bits) * PLANE + flip(my_seat, i, 2)
                if mask or i:
                    query_copy(target, mask).start()

    @pl.when(at_inner == 1)
    def _():
        pl.semaphore_wait(barrier, n // 2)
        for mask in SECOND:
            greet(mask)
        send(FIRST)
        pl.semaphore_wait(barrier, n // 2)
        send(SECOND)

    @pl.when(at_inner == 0)
    def _():
        pl.semaphore_wait(barrier, n)
        for mask in SECOND:
            greet(mask)
        send(OUTER)

    take[...] = jnp.where(
        lax.broadcasted_iota(jnp.int32, (children, slots), 1).astype(jnp.float32) == slot_down,
        jnp.ones((children, slots), jnp.float32),
        jnp.zeros((children, slots), jnp.float32),
    ).astype(jnp.bfloat16)
    landed[me] = outgoing[me]
    for fetch in fetches[2:]:
        fetch.wait()
    blocks(ids, ids, n - 1, id_send, id_recv).wait_recv()
    scale = math.log2(math.e) / math.sqrt(HEAD_WIDTH)

    @pl.loop(0, planes)
    def _(g):
        mask = pick(STEP_OUTER, STEP_INNER, at_inner, g)
        plane = flip(my_plane, mask, bits)
        seats = [plane * PLANE + flip(my_seat, i, 2) for i in range(PLANE)]

        @pl.when(mask > 0)
        def _():
            blocks(outgoing, landed, PLANE, send_sem, recv_sem.at[mask]).wait_recv()

        @pl.when(mask == 0)
        def _():
            blocks(outgoing, landed, PLANE - 1, send_sem, recv_sem.at[0]).wait_recv()

        base = plane * PLANE
        spot = lax.broadcasted_iota(jnp.int32, (capacity, 1), 0).astype(jnp.float32)
        tag_parts = []
        for i in range(PLANE):
            known = ids[base + i]
            number = jnp.zeros((capacity, 1), jnp.float32)
            for p in range(parents - 1):
                smaller = jnp.where(
                    known >= me * parents, jnp.where(known <= me * parents + p, 1.0, 0.0), 0.0
                )
                count = jnp.sum(smaller, axis=1, keepdims=True)
                number = number + jnp.where(spot >= count, 1.0, 0.0)
            tag_parts.append(number)
        tags = jnp.concatenate(tag_parts * group, axis=0)
        belongs = [tags == float(p) for p in range(parents)]
        limit = jnp.full(tags.shape, lengths[parents - 1], jnp.int32)
        for p in range(parents - 1):
            limit = jnp.where(belongs[p], lengths[p], limit)
        live = lax.broadcasted_iota(jnp.int32, (rows * group, span), 1) < limit
        pieces = []
        for j in range(kv_heads):
            at = j * HEAD_WIDTH
            q = jnp.concatenate(
                [
                    landed[
                        pl.ds(base, PLANE), :, (j * group + h) * HEAD_WIDTH:(j * group + h + 1) * HEAD_WIDTH
                    ].reshape(rows, HEAD_WIDTH)
                    for h in range(group)
                ],
                axis=0,
            )
            spread = jnp.concatenate(
                [jnp.where(belongs[p], q, jnp.zeros_like(q)) for p in range(parents)], axis=1
            )
            key_pair = jnp.concatenate(
                [keys[p, :, at:at + HEAD_WIDTH] for p in range(parents)], axis=1
            )
            scores = lax.dot_general(
                spread, key_pair, (((1,), (1,)), ((), ())), preferred_element_type=jnp.float32
            )
            raised = jnp.where(live, jnp.exp2(scores * scale), 0.0)
            totals = jnp.sum(raised, axis=1, keepdims=True)
            soft = raised.astype(jnp.bfloat16)
            value_pair = jnp.concatenate(
                [values[p, :, at:at + HEAD_WIDTH] for p in range(parents)], axis=1
            )
            both = jnp.dot(soft, value_pair, preferred_element_type=jnp.float32)
            summed = both[:, (parents - 1) * HEAD_WIDTH:]
            for p in range(parents - 1):
                summed = jnp.where(
                    belongs[p], both[:, p * HEAD_WIDTH:(p + 1) * HEAD_WIDTH], summed
                )
            answer = (summed / totals).astype(jnp.bfloat16)
            pieces += [answer[h * rows:(h + 1) * rows] for h in range(group)]
        attended = jnp.concatenate(pieces, axis=1)
        theirs = pl.multiple_of(partner * half, HEAD_WIDTH)
        mine = pl.multiple_of(core * half, HEAD_WIDTH)
        part_out[g] = jnp.dot(
            attended, weight[:, pl.ds(theirs, half)], preferred_element_type=jnp.float32
        ).astype(jnp.bfloat16)
        part_copy(g).start()
        own[...] = jnp.dot(
            attended, weight[:, pl.ds(mine, half)], preferred_element_type=jnp.float32
        )
        part_copy(g).wait_recv()
        total = (own[...] + part_in[g].astype(jnp.float32)).astype(jnp.bfloat16)
        result[pl.ds(base, PLANE)] = total.reshape(PLANE, capacity, half)

        @pl.when(mask > 0)
        def _():
            back_copy(seats[0]).start()

        for i in range(1, PLANE):
            back_copy(seats[i]).start()

    back[me] = result[me]
    blocks(ids, ids, n - 1, id_send, id_recv).wait_send()
    blocks(outgoing, landed, n - 1, send_sem, recv_sem.at[0]).wait_send()
    for g in range(planes):
        part_copy(g).wait_send()
    blocks(result, back, n - 1, back_send, back_recv).wait_recv()
    mixed = jnp.dot(
        take[...], back[...].reshape(slots, half), preferred_element_type=jnp.float32
    )
    mixed_ref[...] = mixed.astype(jnp.bfloat16)
    blocks(result, back, n - 1, back_send, back_recv).wait_send()


def exchange(n, capacity, queries, cached_key_rows, cached_value_rows, parent_ids, lengths, residual, out_weight):
    children, columns = queries.shape
    half = residual.shape[1]
    planes = n // PLANE
    anywhere = pl.BlockSpec(memory_space=pltpu.HBM)
    rows = PLANE * capacity
    dma = pltpu.SemaphoreType.DMA

    def held(*shape):
        return pltpu.VMEM(shape, jnp.bfloat16)

    return pl.pallas_call(
        functools.partial(exchange_kernel, n),
        out_shape=jax.ShapeDtypeStruct(residual.shape, jnp.bfloat16),
        in_specs=[anywhere] * 6,
        out_specs=pl.BlockSpec(memory_space=pltpu.VMEM),
        scratch_shapes=[
            held(*queries.shape),
            held(*cached_key_rows.shape),
            held(*cached_value_rows.shape),
            held(*out_weight.shape),
            pltpu.SMEM(lengths.shape, jnp.int32),
            pltpu.VMEM((n, 1, children), jnp.int32),
            held(n, capacity, columns),
            held(n, capacity, columns),
            held(n, capacity, half),
            held(n, capacity, half),
            held(planes, rows, half),
            held(planes, rows, half),
            pltpu.VMEM((rows, half), jnp.float32),
            held(children, n * capacity),
            dma((6,)), dma, dma, dma, dma((planes,)), dma((planes,)), dma((planes,)), dma, dma,
        ],
        compiler_params=pltpu.CompilerParams(
            collective_id=0, has_side_effects=True, vmem_limit_bytes=VMEM_MB << 20
        ),
    )(
        *(
            pltpu.with_memory_space_constraint(operand, pltpu.HBM)
            for operand in (
                queries,
                cached_key_rows,
                cached_value_rows,
                parent_ids.reshape(1, children),
                lengths,
                out_weight,
            )
        )
    )


def local(queries, cached_key_rows, cached_value_rows, parent_ids, lengths, residual, out_weight):
    dp_count = lax.axis_size("dp")
    children = queries.shape[0]
    columns = queries.shape[1]
    kv_heads = cached_key_rows.shape[2] // HEAD_WIDTH
    parents_here = lengths.shape[0]
    capacity = max(2, 2 * children // dp_count)
    half = residual.shape[1]
    tensor_count = lax.axis_size("tensor")
    planes = dp_count // PLANE
    if (
        capacity % 16 == 0
        and children % 128 == 0
        and dp_count % PLANE == 0
        and planes == len(SECOND + FIRST)
        and tensor_count == 2
    ):
        mixed = exchange(
            dp_count, capacity, queries, cached_key_rows, cached_value_rows, parent_ids, lengths, residual, out_weight
        )
        return (residual.astype(jnp.float32) + mixed.astype(jnp.float32)).astype(jnp.bfloat16)
    owner_of = parent_ids // parents_here
    sub_index = parent_ids % parents_here
    slot_count = dp_count * capacity
    order_rows = jnp.arange(children, dtype=jnp.int32)
    earlier = (owner_of[:, None] == owner_of[None, :]) & (order_rows[:, None] > order_rows[None, :])
    slot_rank = jnp.sum(earlier.astype(jnp.int32), axis=1)
    slot_of = owner_of * capacity + slot_rank
    placing = jnp.arange(slot_count, dtype=jnp.int32)[:, None] == slot_of[None, :]
    placing_rows = placing.astype(jnp.bfloat16)
    tag = jnp.broadcast_to((sub_index + 1)[:, None], (children, HEAD_WIDTH)).astype(jnp.bfloat16)
    outgoing = jnp.dot(
        placing_rows,
        jnp.concatenate([queries, tag], axis=1),
        preferred_element_type=jnp.float32,
    ).astype(jnp.bfloat16)
    landed = lax.all_to_all(outgoing, "dp", split_axis=0, concat_axis=0, tiled=True)
    arrived = landed[:, :columns]
    arrived_parent = landed[:, columns].astype(jnp.int32) - 1
    answered = jnp.zeros((slot_count, columns), jnp.bfloat16)
    for parent in range(parents_here):
        answer = attend(
            arrived, cached_key_rows[parent], cached_value_rows[parent], lengths[parent], kv_heads
        )
        answered = jnp.where((arrived_parent == parent)[:, None], answer, answered)
    partial_value = jnp.dot(answered, out_weight, preferred_element_type=jnp.float32)
    mine = lax.axis_index("tensor")
    blocks = partial_value.astype(jnp.bfloat16)
    summed = lax.dynamic_slice_in_dim(blocks, mine * half, half, 1).astype(jnp.float32)
    for step in range(1, tensor_count):
        target = lax.rem(mine + step, tensor_count)
        sent = lax.dynamic_slice_in_dim(blocks, target * half, half, 1)
        ring = [(i, (i + step) % tensor_count) for i in range(tensor_count)]
        summed = summed + lax.ppermute(sent, "tensor", ring).astype(jnp.float32)
    returned = lax.all_to_all(
        summed.astype(jnp.bfloat16), "dp", split_axis=0, concat_axis=0, tiled=True
    )
    mixed = lax.dot_general(
        placing_rows, returned, (((0,), (0,)), ((), ())), preferred_element_type=jnp.float32
    )
    return (residual.astype(jnp.float32) + mixed).astype(jnp.bfloat16)


def solution(mesh):
    placed = (
        P("dp", "tensor"),
        P("dp", None, "tensor"),
        P("dp", None, "tensor"),
        P("dp"),
        P("dp"),
        P("dp", "tensor"),
        P("tensor", None),
    )
    return jax.shard_map(
        local, mesh=mesh, in_specs=placed, out_specs=P("dp", "tensor"), check_vma=False
    )
```

```python
import functools
import math

import jax
import jax.numpy as jnp
from jax import lax
from jax.experimental import pallas as pl
from jax.experimental.pallas import tpu as pltpu
from jax.sharding import PartitionSpec as P

HEAD_WIDTH = 128


def attend(rows, key_block, value_block, prefix_length, kv_heads):
    slot_total, columns = rows.shape
    group_width = columns // (kv_heads * HEAD_WIDTH)
    prefix_span = key_block.shape[0]
    query_head_count = rows.reshape(slot_total, kv_heads, group_width, HEAD_WIDTH)
    key_heads = key_block.reshape(prefix_span, kv_heads, HEAD_WIDTH)
    value_heads = value_block.reshape(prefix_span, kv_heads, HEAD_WIDTH)
    scores = jnp.einsum(
        "sjgd,ljd->jsgl", query_head_count, key_heads, preferred_element_type=jnp.float32
    )
    scores = scores * (1.0 / math.sqrt(HEAD_WIDTH))
    live_mask = jnp.arange(prefix_span, dtype=jnp.int32) < prefix_length
    raised = jnp.where(live_mask, jnp.exp(scores), jnp.zeros((), jnp.float32))
    totals = jnp.sum(raised, axis=-1)
    summed = jnp.einsum(
        "jsgl,ljd->sjgd",
        raised.astype(jnp.bfloat16),
        value_heads,
        preferred_element_type=jnp.float32,
    )
    scaled = summed / jnp.transpose(totals, (1, 0, 2))[..., None]
    return scaled.reshape(slot_total, columns).astype(jnp.bfloat16)

PLANE = 4
MESH = pl.DeviceIdType.MESH
VMEM_MB = 40


FIRST, SECOND, OUTER = (0, 3), (1, 2), (0, 1, 2, 3)
STEP_OUTER, STEP_INNER = (0, 1, 3, 2), (0, 1, 2, 3)


def pick(outer, inner, at_inner, step):
    return sum(
        (o + at_inner * (i - o)) * jnp.where(step == k, 1, 0)
        for k, (o, i) in enumerate(zip(outer, inner))
    )


def flip(number, mask, bits):
    total = 0
    for bit in range(bits):
        unit = 1 << bit
        total = total + ((number // unit) % 2 + (mask // unit) % 2) % 2 * unit
    return total


def exchange_kernel(
    n, query_hbm, key_hbm, value_hbm, id_hbm, length_hbm, weight_hbm, mixed_ref,
    queries, keys, values, weight, lengths, ids, outgoing, landed, result, back,
    part_out, part_in, own, take, fetch_sem, id_send, id_recv, send_sem, recv_sem,
    part_send, part_recv, back_send, back_recv,
):
    me = lax.axis_index("dp")
    core = lax.axis_index("tensor")
    partner = 1 - core
    planes = n // PLANE
    bits = planes.bit_length() - 1
    my_plane, my_seat = me // PLANE, me % PLANE
    children, columns = queries.shape
    capacity = outgoing.shape[1]
    parents, span, _ = keys.shape
    kv_heads = keys.shape[2] // HEAD_WIDTH
    half = result.shape[2]
    group = columns // (kv_heads * HEAD_WIDTH)
    rows = PLANE * capacity
    slots = n * capacity

    fetches = [
        pltpu.make_async_copy(source, target, fetch_sem.at[i])
        for i, (source, target) in enumerate(
            [
                (id_hbm, ids.at[me]),
                (query_hbm, queries),
                (length_hbm, lengths),
                (key_hbm, keys),
                (value_hbm, values),
                (weight_hbm, weight),
            ]
        )
    ]
    for fetch in fetches[:2]:
        fetch.start()

    barrier = pltpu.get_barrier_semaphore()
    at_inner = (my_plane + 1) // 2 % 2

    def greet(mask):
        for i in range(PLANE):
            target = flip(my_plane, mask, bits) * PLANE + flip(my_seat, i, 2)
            if mask or i:
                pl.semaphore_signal(barrier, inc=1, device_id=(target, core), device_id_type=MESH)

    for mask in FIRST:
        greet(mask)
    pl.semaphore_signal(barrier, inc=1, device_id=(me, partner), device_id_type=MESH)
    def remote(source, target, send, recv, device):
        return pltpu.make_async_remote_copy(
            src_ref=source,
            dst_ref=target,
            send_sem=send,
            recv_sem=recv,
            device_id=device,
            device_id_type=MESH,
        )

    def id_copy(target):
        return remote(ids.at[me], ids.at[me], id_send, id_recv, (target, core))

    def query_copy(target, mask):
        return remote(
            outgoing.at[target], landed.at[me], send_sem, recv_sem.at[mask], (target, core)
        )

    def back_copy(target):
        return remote(result.at[target], back.at[me], back_send, back_recv, (target, core))

    def part_copy(g):
        return remote(
            part_out.at[g], part_in.at[g], part_send.at[g], part_recv.at[g], (me, partner)
        )

    def blocks(source, target, count, send, recv):
        return remote(
            source.at[pl.ds(0, count)], target.at[pl.ds(0, count)], send, recv, (me, partner)
        )

    fetches[0].wait()
    square = (children, children)
    across = jnp.broadcast_to(ids[me].astype(jnp.float32), square)
    down = across.T
    owner_across = jnp.floor((across + 0.5) * (1.0 / parents))
    owner_down = jnp.floor((down + 0.5) * (1.0 / parents))
    row_at = lax.broadcasted_iota(jnp.int32, square, 0)
    column_at = lax.broadcasted_iota(jnp.int32, square, 1)
    zero, one = jnp.zeros(square, jnp.float32), jnp.ones(square, jnp.float32)
    kin = owner_across == owner_down
    alike = jnp.where(across == down, one, zero)
    lower = jnp.where(column_at < row_at, alike, zero)
    upper = jnp.where(row_at < column_at, alike, zero)
    before_down = jnp.where(kin, jnp.where(across < down, one, lower), zero)
    before_across = jnp.where(kin, jnp.where(down < across, one, upper), zero)
    slot_down = owner_down[:, :1] * capacity + jnp.sum(before_down, axis=1, keepdims=True)
    slot_across = owner_across[:1] * capacity + jnp.sum(before_across, axis=0, keepdims=True)
    place = jnp.where(
        lax.broadcasted_iota(jnp.int32, (slots, children), 0).astype(jnp.float32) == slot_across,
        jnp.ones((slots, children), jnp.float32),
        jnp.zeros((slots, children), jnp.float32),
    ).astype(jnp.bfloat16)
    fetches[1].wait()
    for fetch in fetches[2:]:
        fetch.start()
    outgoing[...] = (
        jnp.dot(place, queries[...], preferred_element_type=jnp.float32)
        .astype(jnp.bfloat16)
        .reshape(n, capacity, columns)
    )
    def send(masks):
        for mask in masks:
            for i in range(PLANE):
                target = flip(my_plane, mask, bits) * PLANE + flip(my_seat, i, 2)
                if mask or i:
                    id_copy(target).start()
        for mask in masks:
            for i in reversed(range(PLANE)):
                target = flip(my_plane, mask, bits) * PLANE + flip(my_seat, i, 2)
                if mask or i:
                    query_copy(target, mask).start()

    @pl.when(at_inner == 1)
    def _():
        pl.semaphore_wait(barrier, n // 2)
        for mask in SECOND:
            greet(mask)
        send(FIRST)
        pl.semaphore_wait(barrier, n // 2)
        send(SECOND)

    @pl.when(at_inner == 0)
    def _():
        pl.semaphore_wait(barrier, n)
        for mask in SECOND:
            greet(mask)
        send(OUTER)

    take[...] = jnp.where(
        lax.broadcasted_iota(jnp.int32, (children, slots), 1).astype(jnp.float32) == slot_down,
        jnp.ones((children, slots), jnp.float32),
        jnp.zeros((children, slots), jnp.float32),
    ).astype(jnp.bfloat16)
    landed[me] = outgoing[me]
    for fetch in fetches[2:]:
        fetch.wait()
    blocks(ids, ids, n - 1, id_send, id_recv).wait_recv()
    scale = math.log2(math.e) / math.sqrt(HEAD_WIDTH)

    @pl.loop(0, planes)
    def _(g):
        mask = pick(STEP_OUTER, STEP_INNER, at_inner, g)
        plane = flip(my_plane, mask, bits)
        seats = [plane * PLANE + flip(my_seat, i, 2) for i in range(PLANE)]

        @pl.when(mask > 0)
        def _():
            blocks(outgoing, landed, PLANE, send_sem, recv_sem.at[mask]).wait_recv()

        @pl.when(mask == 0)
        def _():
            blocks(outgoing, landed, PLANE - 1, send_sem, recv_sem.at[0]).wait_recv()

        base = plane * PLANE
        spot = lax.broadcasted_iota(jnp.int32, (capacity, 1), 0).astype(jnp.float32)
        tag_parts = []
        for i in range(PLANE):
            known = ids[base + i]
            number = jnp.zeros((capacity, 1), jnp.float32)
            for p in range(parents - 1):
                smaller = jnp.where(
                    known >= me * parents, jnp.where(known <= me * parents + p, 1.0, 0.0), 0.0
                )
                count = jnp.sum(smaller, axis=1, keepdims=True)
                number = number + jnp.where(spot >= count, 1.0, 0.0)
            tag_parts.append(number)
        tags = jnp.concatenate(tag_parts * group, axis=0)
        belongs = [tags == float(p) for p in range(parents)]
        limit = jnp.full(tags.shape, lengths[parents - 1], jnp.int32)
        for p in range(parents - 1):
            limit = jnp.where(belongs[p], lengths[p], limit)
        live = lax.broadcasted_iota(jnp.int32, (rows * group, span), 1) < limit
        pieces = []
        for j in range(kv_heads):
            at = j * HEAD_WIDTH
            q = jnp.concatenate(
                [
                    landed[
                        pl.ds(base, PLANE), :, (j * group + h) * HEAD_WIDTH:(j * group + h + 1) * HEAD_WIDTH
                    ].reshape(rows, HEAD_WIDTH)
                    for h in range(group)
                ],
                axis=0,
            )
            spread = jnp.concatenate(
                [jnp.where(belongs[p], q, jnp.zeros_like(q)) for p in range(parents)], axis=1
            )
            key_pair = jnp.concatenate(
                [keys[p, :, at:at + HEAD_WIDTH] for p in range(parents)], axis=1
            )
            scores = lax.dot_general(
                spread, key_pair, (((1,), (1,)), ((), ())), preferred_element_type=jnp.float32
            )
            raised = jnp.where(live, jnp.exp2(scores * scale), 0.0)
            totals = jnp.sum(raised, axis=1, keepdims=True)
            soft = raised.astype(jnp.bfloat16)
            value_pair = jnp.concatenate(
                [values[p, :, at:at + HEAD_WIDTH] for p in range(parents)], axis=1
            )
            both = jnp.dot(soft, value_pair, preferred_element_type=jnp.float32)
            summed = both[:, (parents - 1) * HEAD_WIDTH:]
            for p in range(parents - 1):
                summed = jnp.where(
                    belongs[p], both[:, p * HEAD_WIDTH:(p + 1) * HEAD_WIDTH], summed
                )
            answer = (summed / totals).astype(jnp.bfloat16)
            pieces += [answer[h * rows:(h + 1) * rows] for h in range(group)]
        attended = jnp.concatenate(pieces, axis=1)
        theirs = pl.multiple_of(partner * half, HEAD_WIDTH)
        mine = pl.multiple_of(core * half, HEAD_WIDTH)
        part_out[g] = jnp.dot(
            attended, weight[:, pl.ds(theirs, half)], preferred_element_type=jnp.float32
        ).astype(jnp.bfloat16)
        part_copy(g).start()
        own[...] = jnp.dot(
            attended, weight[:, pl.ds(mine, half)], preferred_element_type=jnp.float32
        )
        part_copy(g).wait_recv()
        total = (own[...] + part_in[g].astype(jnp.float32)).astype(jnp.bfloat16)
        result[pl.ds(base, PLANE)] = total.reshape(PLANE, capacity, half)

        for i in range(PLANE - 1, 0, -1):
            back_copy(seats[i]).start()

        @pl.when(mask > 0)
        def _():
            back_copy(seats[0]).start()

    back[me] = result[me]
    blocks(ids, ids, n - 1, id_send, id_recv).wait_send()
    blocks(outgoing, landed, n - 1, send_sem, recv_sem.at[0]).wait_send()
    for g in range(planes):
        part_copy(g).wait_send()
    blocks(result, back, n - 1, back_send, back_recv).wait_recv()
    mixed = jnp.dot(
        take[...], back[...].reshape(slots, half), preferred_element_type=jnp.float32
    )
    mixed_ref[...] = mixed.astype(jnp.bfloat16)
    blocks(result, back, n - 1, back_send, back_recv).wait_send()


def exchange(n, capacity, queries, cached_key_rows, cached_value_rows, parent_ids, lengths, residual, out_weight):
    children, columns = queries.shape
    half = residual.shape[1]
    planes = n // PLANE
    anywhere = pl.BlockSpec(memory_space=pltpu.HBM)
    rows = PLANE * capacity
    dma = pltpu.SemaphoreType.DMA

    def held(*shape):
        return pltpu.VMEM(shape, jnp.bfloat16)

    return pl.pallas_call(
        functools.partial(exchange_kernel, n),
        out_shape=jax.ShapeDtypeStruct(residual.shape, jnp.bfloat16),
        in_specs=[anywhere] * 6,
        out_specs=pl.BlockSpec(memory_space=pltpu.VMEM),
        scratch_shapes=[
            held(*queries.shape),
            held(*cached_key_rows.shape),
            held(*cached_value_rows.shape),
            held(*out_weight.shape),
            pltpu.SMEM(lengths.shape, jnp.int32),
            pltpu.VMEM((n, 1, children), jnp.int32),
            held(n, capacity, columns),
            held(n, capacity, columns),
            held(n, capacity, half),
            held(n, capacity, half),
            held(planes, rows, half),
            held(planes, rows, half),
            pltpu.VMEM((rows, half), jnp.float32),
            held(children, n * capacity),
            dma((6,)), dma, dma, dma, dma((planes,)), dma((planes,)), dma((planes,)), dma, dma,
        ],
        compiler_params=pltpu.CompilerParams(
            collective_id=0, has_side_effects=True, vmem_limit_bytes=VMEM_MB << 20
        ),
    )(
        *(
            pltpu.with_memory_space_constraint(operand, pltpu.HBM)
            for operand in (
                queries,
                cached_key_rows,
                cached_value_rows,
                parent_ids.reshape(1, children),
                lengths,
                out_weight,
            )
        )
    )


def local(queries, cached_key_rows, cached_value_rows, parent_ids, lengths, residual, out_weight):
    dp_count = lax.axis_size("dp")
    children = queries.shape[0]
    columns = queries.shape[1]
    kv_heads = cached_key_rows.shape[2] // HEAD_WIDTH
    parents_here = lengths.shape[0]
    capacity = max(2, 2 * children // dp_count)
    half = residual.shape[1]
    tensor_count = lax.axis_size("tensor")
    planes = dp_count // PLANE
    if (
        capacity % 16 == 0
        and children % 128 == 0
        and dp_count % PLANE == 0
        and planes == len(SECOND + FIRST)
        and tensor_count == 2
    ):
        mixed = exchange(
            dp_count, capacity, queries, cached_key_rows, cached_value_rows, parent_ids, lengths, residual, out_weight
        )
        return (residual.astype(jnp.float32) + mixed.astype(jnp.float32)).astype(jnp.bfloat16)
    owner_of = parent_ids // parents_here
    sub_index = parent_ids % parents_here
    slot_count = dp_count * capacity
    order_rows = jnp.arange(children, dtype=jnp.int32)
    earlier = (owner_of[:, None] == owner_of[None, :]) & (order_rows[:, None] > order_rows[None, :])
    slot_rank = jnp.sum(earlier.astype(jnp.int32), axis=1)
    slot_of = owner_of * capacity + slot_rank
    placing = jnp.arange(slot_count, dtype=jnp.int32)[:, None] == slot_of[None, :]
    placing_rows = placing.astype(jnp.bfloat16)
    tag = jnp.broadcast_to((sub_index + 1)[:, None], (children, HEAD_WIDTH)).astype(jnp.bfloat16)
    outgoing = jnp.dot(
        placing_rows,
        jnp.concatenate([queries, tag], axis=1),
        preferred_element_type=jnp.float32,
    ).astype(jnp.bfloat16)
    landed = lax.all_to_all(outgoing, "dp", split_axis=0, concat_axis=0, tiled=True)
    arrived = landed[:, :columns]
    arrived_parent = landed[:, columns].astype(jnp.int32) - 1
    answered = jnp.zeros((slot_count, columns), jnp.bfloat16)
    for parent in range(parents_here):
        answer = attend(
            arrived, cached_key_rows[parent], cached_value_rows[parent], lengths[parent], kv_heads
        )
        answered = jnp.where((arrived_parent == parent)[:, None], answer, answered)
    partial_value = jnp.dot(answered, out_weight, preferred_element_type=jnp.float32)
    mine = lax.axis_index("tensor")
    blocks = partial_value.astype(jnp.bfloat16)
    summed = lax.dynamic_slice_in_dim(blocks, mine * half, half, 1).astype(jnp.float32)
    for step in range(1, tensor_count):
        target = lax.rem(mine + step, tensor_count)
        sent = lax.dynamic_slice_in_dim(blocks, target * half, half, 1)
        ring = [(i, (i + step) % tensor_count) for i in range(tensor_count)]
        summed = summed + lax.ppermute(sent, "tensor", ring).astype(jnp.float32)
    returned = lax.all_to_all(
        summed.astype(jnp.bfloat16), "dp", split_axis=0, concat_axis=0, tiled=True
    )
    mixed = lax.dot_general(
        placing_rows, returned, (((0,), (0,)), ((), ())), preferred_element_type=jnp.float32
    )
    return (residual.astype(jnp.float32) + mixed).astype(jnp.bfloat16)


def solution(mesh):
    placed = (
        P("dp", "tensor"),
        P("dp", None, "tensor"),
        P("dp", None, "tensor"),
        P("dp"),
        P("dp"),
        P("dp", "tensor"),
        P("tensor", None),
    )
    return jax.shard_map(
        local, mesh=mesh, in_specs=placed, out_specs=P("dp", "tensor"), check_vma=False
    )
```
